32 devices in a mesh: parts: 2 (over x), genes: 8 (over z, y), samples: 2 (over core).
Axes of the slice: x: 2, y: 2, z: 4, core: 2. Of those that a mesh axis runs over, the one named last changes fastest.
Arguments:
- dosage: bfloat16 [32768, 2048], P(('parts', 'genes'), 'samples'), parts along dimension 0, may hold values from -6 to 6
- expression: bfloat16 [128, 2048], P(('parts', 'genes'), 'samples'), parts along dimension 0, may hold values from -6 to 6
- intron_counts: bfloat16 [4096, 2560], P(('parts', 'samples', 'genes')), parts along dimension 0, may hold values from 1 to 100
- cluster_sizes: int32 [128, 8], P('parts'), parts along dimension 0, may hold values from 1 to 12, 40 in all within a row
- valid_mask: int32 [128, 40], P('parts'), parts along dimension 0, may hold values 0 or 1
- gene_block: int32 [128], P('parts'), parts along dimension 0, may hold values from 0 to 63, each once
- window_start: int32 [128], P(('parts', 'genes')), parts along dimension 0, may hold values from 0 to 1024, as said below
Outputs:
- assoc: bfloat16 [128, 41, 2048], P(('parts', 'genes'), None, 'samples'), parts along dimension 0
The draws below stay inside these ranges and needn't reach their ends.
There are 2 independent parts, one for each index of `parts`. The reference program is written for one: setup_inputs(seed, part) draws one part's arguments, and reference() takes and returns one part's arrays. A program takes and returns all parts, laid end to end along the dimension named above; each array names one. Nothing has to cross between parts.
Inputs may be any that keep to these rules, and one draw needn't show every extreme that they name: Every window_start is a multiple of 128 and at most 1024; some gene reaches 1024 in every draw. `gene_block`: a permutation of the genes. `cluster_sizes`: each row sums to 40.
All inputs are finite; a program needn't handle non-finite values.
Results may differ from the reference program's by a relative error of at most 0.0058.
Values may be sent and summed in bfloat16 or wider, within the bound.
A program may use at most 64 MiB of HBM per device.

```python
import math
import jax
import jax.numpy as jnp
import numpy as np
from jax import lax

GENE_DEV = 8
W = 2048
SLOTS = 40
CLUST = 8
CL_MOST = 12
SPILL = 1024
ALIGN = 128
PHEN = 41
GENES = 64
SAMP = 2048
VARIANTS = 16384
INTRONS = 2560
N_GENES = 8


def draw_window_start(key, part):
    draw_starts, draw_pick = jax.random.split(jax.random.fold_in(key, 7))
    starts = jax.random.randint(draw_starts, (GENES,), 0, SPILL // ALIGN + 1, dtype=jnp.int32) * ALIGN
    chosen = jax.random.randint(draw_pick, (), 0, GENES, dtype=jnp.int32)
    return jnp.where(jnp.arange(GENES, dtype=jnp.int32) == chosen, SPILL, starts).astype(jnp.int32)


def plant(array, key, least, high):
    spot = [jax.random.randint(jax.random.fold_in(key, axis), (), 0, length) for axis, length in enumerate(array.shape)]
    main_axis = array.shape.index(max(array.shape))
    neighbour = spot[:main_axis] + [(spot[main_axis] + 1) % array.shape[main_axis]] + spot[main_axis + 1:]
    return array.at[tuple(spot)].set(least).at[tuple(neighbour)].set(high)


def steps_of(own_key, shape, cuts, least, high):
    def one(dim, parts):
        heights = jax.random.uniform(jax.random.fold_in(jax.random.fold_in(own_key, 6), dim), (parts,), jnp.float32, least / len(cuts), high / len(cuts))
        return jnp.repeat(jnp.exp(heights), shape[dim] // parts).reshape((-1,) + (1,) * (len(shape) - dim - 1))

    factor_of = one(*cuts[0])
    for cut in cuts[1:]:
        factor_of = factor_of * one(*cut)
    return factor_of


def split_up(amount, total, most, lean):
    loads = [(1 << 20) // math.isqrt(rank ** lean) + 1 for rank in range(2, amount + 1)]
    spare, given = total - most - (amount - 1), [1] * (amount - 1)
    while spare > 0:
        movable = [i for i in range(amount - 1) if given[i] < most]
        mass, left = sum([loads[i] for i in movable]), spare
        for i in movable:
            more = min(most - given[i], max(1, left * loads[i] // mass), spare)
            given[i] = given[i] + more
            spare = spare - more
    return np.array([most] + given)


def uneven(key, count, total, bound, slope):
    if count == 2:
        one = jax.random.randint(key, (), max(1, total - bound), min(bound, total - 1) + 1)
        return jnp.stack([one, total - one])
    sizes = jnp.asarray(split_up(count, total, bound, slope), jnp.int32)
    couples = (count - 1) // 2
    giver, taker = sizes[1:1 + 2 * couples:2], sizes[2:2 + 2 * couples:2]
    slack = jnp.minimum(giver - 1, bound - taker)
    passed = jax.random.randint(jax.random.fold_in(key, 1), (couples,), 0, 1 << 20) % (slack + 1)
    sizes = sizes.at[1:1 + 2 * couples:2].set(giver - passed).at[2:2 + 2 * couples:2].set(taker + passed)
    return sizes[jax.random.permutation(jax.random.fold_in(key, 2), count)]


def scatter_about(own_key, shape, scale, bound, shards=(), held_as=jnp.bfloat16):
    entries = scale * jax.random.normal(own_key, shape, jnp.float32)
    if shards:
        entries = entries * steps_of(own_key, shape, shards, -0.22, 0.18)
    return jnp.clip(entries, -bound, bound).astype(held_as)


def setup_inputs(seed: int = 0, part: int = 0) -> dict:
    splits = jax.random.split(jax.random.key(seed), 8)
    own_keys = jax.random.split(jax.random.fold_in(splits[7], part), 8)
    dosage = scatter_about(own_keys[0], (VARIANTS, SAMP), 1.0, 6.0, ((0, 8), (1, 2)))
    expression = scatter_about(own_keys[1], (GENES, SAMP), 1.0, 6.0, ((0, 8), (1, 2)))
    intron_counts = jnp.clip(jnp.exp(math.log(100.0) - 4.6051702 * jax.random.uniform(own_keys[2], (SAMP, INTRONS), jnp.float32) ** steps_of(own_keys[2], (SAMP, INTRONS), ((0, 16),), -0.2, 0.2)), 1.0, 100.0).astype(jnp.bfloat16)
    cluster_sizes = jax.vmap(lambda own: uneven(own, CLUST, SLOTS, CL_MOST, 2))(jax.random.split(own_keys[3], GENES)).reshape((GENES, CLUST)).astype(jnp.int32)
    valid_mask = plant((jax.random.randint(own_keys[4], (GENES, SLOTS), 0, 4) < 3).astype(jnp.int32), jax.random.fold_in(own_keys[4], 1), 0, 1)
    gene_block = jax.random.permutation(own_keys[5], GENES).astype(jnp.int32)
    window_start = draw_window_start(jax.random.fold_in(jax.random.fold_in(splits[7], part), 71), part)
    return dict(dosage=dosage, expression=expression, intron_counts=intron_counts, cluster_sizes=cluster_sizes, valid_mask=valid_mask, gene_block=gene_block, window_start=window_start)


def cluster_ratios(counts, cluster_sizes, valid_mask):
    cluster_ends = jnp.cumsum(cluster_sizes, axis=1, dtype=jnp.int32)
    slot_index = jnp.arange(SLOTS, dtype=jnp.int32)
    cluster_id = lax.optimization_barrier(jnp.sum((cluster_ends[:, None, :] <= slot_index[None, :, None]).astype(jnp.int32), axis=2, dtype=jnp.int32))
    same_cluster = (cluster_id[:, :, None] == cluster_id[:, None, :]).astype(jnp.float32)
    live_counts = counts * valid_mask.astype(jnp.float32)[None, :, :]
    cluster_total = jnp.einsum('sgj,gjk->sgk', live_counts, same_cluster, precision=lax.Precision.HIGHEST)
    return (live_counts / jnp.maximum(cluster_total, 1.0)).astype(jnp.bfloat16)

def tile_window(owner_block, offset, width):
    leading = owner_block.shape[:-1]
    tiles = owner_block.reshape(leading + (owner_block.shape[-1] // ALIGN, ALIGN))
    first_tile = (offset // ALIGN).astype(jnp.int32)
    piece = lax.dynamic_slice_in_dim(tiles, first_tile, width // ALIGN, len(leading))
    return piece.reshape(leading + (width,))

def window_slices(product, row_sum, row_square, starts):

    def window_of(owner_block, offset):
        return tile_window(owner_block, offset, W)
    cross_part = jax.vmap(window_of, in_axes=(0, 0))(product, starts)
    sum_part = jax.vmap(window_of, in_axes=(None, 0))(row_sum, starts)
    square_part = jax.vmap(window_of, in_axes=(None, 0))(row_square, starts)
    return (cross_part, sum_part, square_part)

def finish_stats(cross_part, sum_part, square_part, phen_sum, phen_square, sample_count):
    numerator = cross_part - sum_part[:, None, :] * phen_sum[:, :, None] / sample_count
    dose_var = jnp.maximum(square_part - sum_part * sum_part / sample_count, 1.0)
    pheno_var = jnp.maximum(phen_square - phen_sum * phen_sum / sample_count, 1.0)
    return (numerator * lax.rsqrt(dose_var)[:, None, :] * lax.rsqrt(pheno_var)[:, :, None]).astype(jnp.bfloat16)

def reference(dosage, expression, intron_counts, cluster_sizes, valid_mask, gene_block, window_start):
    padded = jnp.concatenate([dosage, jnp.zeros((SPILL, SAMP), jnp.bfloat16)], axis=0)
    stored = intron_counts.reshape(SAMP, GENES, SLOTS)

    def owner_stats(owner_index):
        gene_ids = owner_index * GENE_DEV + jnp.arange(GENE_DEV, dtype=jnp.int32)
        dose_rows = lax.dynamic_slice_in_dim(padded, owner_index * W, W + SPILL, 0)
        counts = jnp.take(stored, gene_block[gene_ids], axis=1).astype(jnp.float32)
        ratios = cluster_ratios(counts, cluster_sizes[gene_ids], valid_mask[gene_ids])
        expr_rows = lax.dynamic_slice_in_dim(expression, owner_index * GENE_DEV, GENE_DEV, 0)
        pheno_panel = jnp.concatenate([expr_rows.T[:, :, None], ratios], axis=2).reshape(SAMP, GENE_DEV * PHEN)
        product = lax.dot_general(pheno_panel, dose_rows, (((0,), (1,)), ((), ())), preferred_element_type=jnp.float32)
        product = product.reshape(GENE_DEV, PHEN, W + SPILL)
        dose_float = dose_rows.astype(jnp.float32)
        row_sum = lax.optimization_barrier(jnp.sum(dose_float, axis=1))
        row_square = lax.optimization_barrier(jnp.sum(dose_float * dose_float, axis=1))
        pheno_float = pheno_panel.astype(jnp.float32)
        phen_sum = lax.optimization_barrier(jnp.sum(pheno_float, axis=0)).reshape(GENE_DEV, PHEN)
        phen_square = lax.optimization_barrier(jnp.sum(pheno_float * pheno_float, axis=0)).reshape(GENE_DEV, PHEN)
        cross_part, sum_part, square_part = window_slices(product, row_sum, row_square, window_start[gene_ids])
        return finish_stats(cross_part, sum_part, square_part, phen_sum, phen_square, float(SAMP))
    result = lax.map(owner_stats, jnp.arange(N_GENES, dtype=jnp.int32))
    return result.reshape(GENES, PHEN, W)
```

```python
import functools

import jax
import jax.numpy as jnp
from jax import lax
from jax.experimental import pallas as pl
from jax.experimental.pallas import tpu as pltpu
from jax.sharding import PartitionSpec as P

LANE = 128
SPILL = 1024
MESH = pl.DeviceIdType.MESH


def lane_tiles_sum(value):
    total = value[:, :LANE]
    for t in range(1, value.shape[1] // LANE):
        total = total + value[:, t * LANE : (t + 1) * LANE]
    return total


def kernel(
    n, genes, slots, starts_ref, block_ref, counts_ref, mix_ref, expr_ref, dose_hbm, out_ref,
    dose, stage, sendbuf, recv, halo, halo_expr, pheno, hpheno, prod, hprod, hprod_in,
    sel_out, sel_in, own_res, halo_full, dstat, dstat_in, pstat, pstat_in, hstat, hstat_in,
    hres, hres_in, win, dose_sem, a2a_send, a2a_recv, fwd_send, fwd_recv, pair_send, pair_recv,
    back_send, back_recv,
):
    me = lax.axis_index("genes")
    core = lax.axis_index("samples")
    other = 1 - core
    rows, samp = dose.shape
    phen = slots + 1
    width = rows // 2
    half = SPILL // 2
    intron_rows = slots * genes
    all_rows = phen * genes
    blk = counts_ref.shape[2]
    count = float(2 * samp)
    shift = n // 2

    dose_copy = pltpu.make_async_copy(dose_hbm, dose, dose_sem)
    dose_copy.start()

    barrier = pltpu.get_barrier_semaphore()

    def greet(k, carry):
        there = lax.rem(me + k, n)
        pl.semaphore_signal(
            barrier, inc=1, device_id={"genes": there, "samples": core}, device_id_type=MESH
        )
        pl.semaphore_signal(
            barrier, inc=1, device_id={"genes": there, "samples": other}, device_id_type=MESH
        )
        return carry

    lax.fori_loop(1, n, greet, 0)
    pl.semaphore_signal(barrier, inc=1, device_id={"samples": other}, device_id_type=MESH)

    def a2a(owner, source):
        return pltpu.make_async_remote_copy(
            src_ref=sendbuf.at[owner], dst_ref=recv.at[source],
            send_sem=a2a_send.at[owner], recv_sem=a2a_recv.at[source],
            device_id={"genes": owner}, device_id_type=MESH,
        )

    def make_block(owner):
        for g in range(genes):
            gene = owner * genes + g
            cnt = counts_ref[block_ref[gene]].astype(jnp.bfloat16)
            both = jnp.dot(mix_ref[gene], cnt, preferred_element_type=jnp.float32)
            ratio = both[slots:] / jnp.maximum(both[:slots], 1.0)
            stage[pl.ds(g, slots, stride=genes), :] = ratio
        sendbuf[owner] = stage[...].astype(jnp.bfloat16)

    make_block(lax.rem(me + shift, n))
    pl.semaphore_wait(barrier, 2 * n - 1)

    def ratio_step(k, carry):
        make_block(lax.rem(me + shift + k, n))

        @pl.when(k - 1 != n - shift)
        def _():
            a2a(lax.rem(me + shift + k - 1, n), me).start()

        return carry

    lax.fori_loop(1, n, ratio_step, 0)
    a2a(lax.rem(me + shift + n - 1, n), me).start()

    dose_copy.wait()
    dstat[:, rows:] = jnp.zeros((16, SPILL), jnp.float32)
    ones = jnp.ones((8, LANE), jnp.float32)
    chunk = 256

    def dose_stat(k, carry):
        at = pl.multiple_of(k * chunk, chunk)
        value = dose[pl.ds(at, chunk), :].astype(jnp.float32)
        dims = (((1,), (1,)), ((), ()))
        for slot, part in ((0, value), (8, value * value)):
            dstat[slot : slot + 8, pl.ds(at, chunk)] = lax.dot_general(
                ones, lane_tiles_sum(part), dims, precision=lax.Precision.HIGHEST,
                preferred_element_type=jnp.float32,
            )
        return carry

    lax.fori_loop(0, rows // chunk, dose_stat, 0)

    def pair(k, src, dst):
        return pltpu.make_async_remote_copy(
            src_ref=src, dst_ref=dst, send_sem=pair_send.at[k], recv_sem=pair_recv.at[k],
            device_id={"samples": other}, device_id_type=MESH,
        )

    def fwd(src, dst, k):
        return pltpu.make_async_remote_copy(
            src_ref=src, dst_ref=dst, send_sem=fwd_send.at[k], recv_sem=fwd_recv.at[k],
            device_id={"genes": lax.rem(me + 1, n)}, device_id_type=MESH,
        )

    has_next = me < n - 1
    has_prev = me > 0

    @pl.when(has_next)
    def _():
        fwd(expr_ref, halo_expr, n).start()
        fwd(sendbuf.at[me], halo.at[me], me).start()

    def relay(k, carry):
        source = lax.rem(me + 2 * n - shift - k, n)

        @pl.when(k != n - shift)
        def _():
            a2a(source, source).wait_recv()

            @pl.when(has_next)
            def _():
                fwd(recv.at[source], halo.at[source], source).start()

        return carry

    dstat_pair = pair(0, dstat, dstat_in)
    dstat_pair.start()
    lax.fori_loop(0, n, relay, 0)
    recv[me] = sendbuf[me]

    def pack(blocks, expr_rows, target, stat):
        for i in range(n):
            target[:intron_rows, i * blk : (i + 1) * blk] = blocks[i]
        target[intron_rows:, :] = expr_rows[...]
        value = target[...].astype(jnp.float32)
        stat[0] = lane_tiles_sum(value)
        stat[1] = lane_tiles_sum(value * value)

    pack(recv, expr_ref, pheno, pstat)
    pstat_pair = pair(1, pstat, pstat_in)

    dims = (((1,), (1,)), ((), ()))
    prod[:, rows:] = jnp.zeros((all_rows, SPILL), jnp.float32)

    def own_dot(k, carry):
        at = pl.multiple_of(k * chunk, chunk)
        prod[:, pl.ds(at, chunk)] = lax.dot_general(
            pheno[...], dose[pl.ds(at, chunk), :], dims, preferred_element_type=jnp.float32
        )
        return carry

    lax.fori_loop(0, rows // chunk, own_dot, 0)
    pstat_pair.start()

    lane_gene = lax.broadcasted_iota(jnp.int32, (genes, LANE), 0)
    starts = jnp.zeros((genes, LANE), jnp.int32)
    for g in range(genes):
        starts = jnp.where(lane_gene == g, starts_ref[g], starts)
    steps = SPILL // LANE
    at_step = [starts == s * LANE for s in range(steps)]

    def windows(source, row, base):
        tiles = []
        for t in range((width + SPILL) // LANE):
            at = pl.multiple_of(base + t * LANE, LANE)
            tiles.append(source[pl.ds(row, genes), pl.ds(at, LANE)])
        picked = []
        for t in range(width // LANE):
            tile = tiles[t + steps]
            for s in range(steps):
                tile = jnp.where(at_step[s], tiles[t + s], tile)
            picked.append(tile)
        return picked

    def select_out(p, carry):
        row = pl.multiple_of(p * genes, genes)
        for t, tile in enumerate(windows(prod, row, other * width)):
            sel_out[pl.ds(row, genes), t * LANE : (t + 1) * LANE] = tile
        return carry

    lax.fori_loop(0, phen, select_out, 0)
    sel_pair = pair(2, sel_out, sel_in)
    sel_pair.start()

    dstat_pair.wait_recv()
    dstat_pair.wait_send()
    dstat[...] = dstat[...] + dstat_in[...]

    def scales(stat, stat_in, row):
        total = jnp.sum(stat[0, pl.ds(row, genes), :] + stat_in[0, pl.ds(row, genes), :], axis=1, keepdims=True)
        square = jnp.sum(stat[1, pl.ds(row, genes), :] + stat_in[1, pl.ds(row, genes), :], axis=1, keepdims=True)
        return total / count, lax.rsqrt(jnp.maximum(square - total * total / count, 1.0))

    def dose_scale(total, square):
        return lax.rsqrt(jnp.maximum(square - total * total / count, 1.0))

    hstat_pair = pair(3, hstat, hstat_in)
    hprod_pair = pair(4, hprod.at[other], hprod_in)
    back = pltpu.make_async_remote_copy(
        src_ref=hres, dst_ref=hres_in.at[core], send_sem=back_send, recv_sem=back_recv.at[core],
        device_id={"genes": lax.rem(me + n - 1, n), "samples": 1}, device_id_type=MESH,
    )

    @pl.when(has_prev)
    def _():
        fwd(expr_ref, halo_expr, n).wait_recv()

        def arrive(k, carry):
            fwd(recv.at[k], halo.at[k], k).wait_recv()
            return carry

        lax.fori_loop(0, n, arrive, 0)
        pack(halo, halo_expr, hpheno, hstat)

        def halo_dot(k, carry):
            at = pl.multiple_of(k * half, half)
            hprod[k] = lax.dot_general(
                hpheno[...], dose[pl.ds(at, half), :], dims, preferred_element_type=jnp.float32
            )
            return carry

        lax.fori_loop(0, 2, halo_dot, 0)
        hstat_pair.start()
        hprod_pair.start()

    pstat_pair.wait_recv()
    sel_pair.wait_recv()
    win_sum = windows(dstat, 0, core * width)
    win_square = windows(dstat, 8, core * width)
    for t in range(width // LANE):
        cols = slice(t * LANE, (t + 1) * LANE)
        win[0:8, cols] = win_sum[t]
        win[8:16, cols] = dose_scale(win_sum[t], win_square[t])

    @pl.when(has_prev)
    def _():
        hstat_pair.wait_recv()
        hprod_pair.wait_recv()
        at = pl.multiple_of(core * half, half)
        sums = dstat[0:8, pl.ds(at, half)]
        scale = dose_scale(sums, dstat[8:16, pl.ds(at, half)])

        def halo_out(p, carry):
            row = pl.multiple_of(p * genes, genes)
            mean, inv = scales(hstat, hstat_in, row)
            cross = hprod[core, pl.ds(row, genes), :] + hprod_in[pl.ds(row, genes), :]
            hres[p] = ((cross - sums * mean) * scale * inv).astype(jnp.bfloat16)
            return carry

        lax.fori_loop(0, phen, halo_out, 0)
        back.start()

    def own_out(p, carry):
        row = pl.multiple_of(p * genes, genes)
        mean, inv = scales(pstat, pstat_in, row)
        for t, tile in enumerate(windows(prod, row, core * width)):
            cols = slice(t * LANE, (t + 1) * LANE)
            cross = tile + sel_in[pl.ds(row, genes), cols]
            own_res[pl.ds(row, genes), cols] = (cross - win[0:8, cols] * mean) * win[8:16, cols] * inv
        return carry

    lax.fori_loop(0, phen, own_out, 0)
    takes_halo = jnp.logical_and(has_next, core == 1)

    @pl.when(takes_halo)
    def _():
        for side in range(2):
            pltpu.make_async_remote_copy(
                src_ref=hres, dst_ref=hres_in.at[side], send_sem=back_send,
                recv_sem=back_recv.at[side],
                device_id={"genes": lax.rem(me + n - 1, n), "samples": 1}, device_id_type=MESH,
            ).wait_recv()
        halo_full[:, :width] = jnp.zeros((all_rows, width), jnp.float32)

        def widen(p, carry):
            row = pl.multiple_of(p * genes, genes)
            for side in range(2):
                halo_full[pl.ds(row, genes), width + side * half : width + (side + 1) * half] = (
                    hres_in[side, p].astype(jnp.float32)
                )
            return carry

        lax.fori_loop(0, phen, widen, 0)

        def add_halo(p, carry):
            row = pl.multiple_of(p * genes, genes)
            for t, tile in enumerate(windows(halo_full, row, 0)):
                cols = slice(t * LANE, (t + 1) * LANE)
                out_ref[lax.rem(p + 1, phen), :, cols] = (
                    own_res[pl.ds(row, genes), cols] + tile
                ).astype(jnp.bfloat16)
            return carry

        lax.fori_loop(0, phen, add_halo, 0)

    @pl.when(jnp.logical_not(takes_halo))
    def _():
        def plain(p, carry):
            row = pl.multiple_of(p * genes, genes)
            out_ref[lax.rem(p + 1, phen)] = own_res[pl.ds(row, genes), :].astype(jnp.bfloat16)
            return carry

        lax.fori_loop(0, phen, plain, 0)

    def drain(k, carry):
        a2a(lax.rem(me + k, n), me).wait_send()
        return carry

    lax.fori_loop(1, n, drain, 0)
    pstat_pair.wait_send()
    sel_pair.wait_send()

    @pl.when(has_next)
    def _():
        fwd(expr_ref, halo_expr, n).wait_send()

        def drain_fwd(k, carry):
            fwd(recv.at[k], halo.at[k], k).wait_send()
            return carry

        lax.fori_loop(0, n, drain_fwd, 0)

    @pl.when(has_prev)
    def _():
        hstat_pair.wait_send()
        hprod_pair.wait_send()
        back.wait_send()


def mixing(cluster_sizes, valid_mask):
    slots = valid_mask.shape[1]
    clusters = cluster_sizes.shape[1]
    slot = jnp.arange(slots, dtype=jnp.int32)
    ends = []
    for c in range(clusters):
        ends.append(cluster_sizes[:, c] + (ends[-1] if c else 0))
    cluster_id = sum((end[:, None] <= slot[None, :]).astype(jnp.int32) for end in ends)
    same = cluster_id[:, :, None] == cluster_id[:, None, :]
    diag = jnp.broadcast_to((slot[:, None] == slot[None, :])[None], same.shape)
    both = jnp.concatenate([same, diag], axis=1)
    return jnp.where(both, valid_mask[:, None, :], 0).astype(jnp.bfloat16)


def shards(dosage, expression, intron_counts, cluster_sizes, valid_mask, gene_block, window_start):
    n = lax.axis_size("genes")
    rows, samp = dosage.shape
    genes = expression.shape[0]
    slots = valid_mask.shape[1]
    blk = intron_counts.shape[0]
    phen = slots + 1
    all_rows = phen * genes
    width = rows // 2
    half = SPILL // 2
    counts_t = intron_counts.T.astype(jnp.float32).reshape(n * genes, slots, blk)
    mix = mixing(cluster_sizes, valid_mask)
    vmem = pl.BlockSpec(memory_space=pltpu.VMEM)
    smem = pl.BlockSpec(memory_space=pltpu.SMEM)
    f32, bf16 = jnp.float32, jnp.bfloat16
    dma = pltpu.SemaphoreType.DMA
    result = pl.pallas_call(
        functools.partial(kernel, n, genes, slots),
        out_shape=jax.ShapeDtypeStruct((phen, genes, width), bf16),
        in_specs=[smem, smem, vmem, vmem, vmem, pl.BlockSpec(memory_space=pl.ANY)],
        out_specs=vmem,
        scratch_shapes=[
            pltpu.VMEM((rows, samp), bf16),
            pltpu.VMEM((slots * genes, blk), f32),
            pltpu.VMEM((n, slots * genes, blk), bf16),
            pltpu.VMEM((n, slots * genes, blk), bf16),
            pltpu.VMEM((n, slots * genes, blk), bf16),
            pltpu.VMEM((genes, samp), bf16),
            pltpu.VMEM((all_rows, samp), bf16),
            pltpu.VMEM((all_rows, samp), bf16),
            pltpu.VMEM((all_rows, rows + SPILL), f32),
            pltpu.VMEM((2, all_rows, half), f32),
            pltpu.VMEM((all_rows, half), f32),
            pltpu.VMEM((all_rows, width), f32),
            pltpu.VMEM((all_rows, width), f32),
            pltpu.VMEM((all_rows, width), f32),
            pltpu.VMEM((all_rows, width + SPILL), f32),
            pltpu.VMEM((16, rows + SPILL), f32),
            pltpu.VMEM((16, rows + SPILL), f32),
            pltpu.VMEM((2, all_rows, LANE), f32),
            pltpu.VMEM((2, all_rows, LANE), f32),
            pltpu.VMEM((2, all_rows, LANE), f32),
            pltpu.VMEM((2, all_rows, LANE), f32),
            pltpu.VMEM((phen, genes, half), bf16),
            pltpu.VMEM((2, phen, genes, half), bf16),
            pltpu.VMEM((16, width), f32),
            dma, dma((n,)), dma((n,)), dma((n + 1,)), dma((n + 1,)), dma((5,)), dma((5,)),
            dma, dma((2,)),
        ],
        compiler_params=pltpu.CompilerParams(
            collective_id=0, has_side_effects=True, vmem_limit_bytes=62 * 1024 * 1024
        ),
    )(window_start, gene_block, counts_t, mix, expression, dosage)
    return jnp.transpose(result, (1, 0, 2))


def solution(mesh):
    in_specs = (
        P(("parts", "genes"), "samples"),
        P(("parts", "genes"), "samples"),
        P(("parts", "samples", "genes"), None),
        P("parts", None),
        P("parts", None),
        P("parts"),
        P(("parts", "genes")),
    )
    out_specs = P(("parts", "genes"), None, "samples")
    return jax.shard_map(shards, mesh=mesh, in_specs=in_specs, out_specs=out_specs, check_vma=False)
```

```python
import functools

import jax
import jax.numpy as jnp
from jax import lax
from jax.experimental import pallas as pl
from jax.experimental.pallas import tpu as pltpu
from jax.sharding import PartitionSpec as P

LANE = 128
SPILL = 1024
MESH = pl.DeviceIdType.MESH


def lane_tiles_sum(value):
    total = value[:, :LANE]
    for t in range(1, value.shape[1] // LANE):
        total = total + value[:, t * LANE : (t + 1) * LANE]
    return total


def kernel(
    n, genes, slots, starts_ref, block_ref, counts_ref, sizes_ref, valid_ref, expr_ref, dose_hbm, out_ref,
    dose, ids, stage, sendbuf, recv, halo, halo_expr, pheno, hpheno, prod, hprod, hprod_in,
    sel_out, sel_in, own_res, halo_full, dstat, dstat_in, pstat, pstat_in, hstat, hstat_in,
    hres, hres_in, win, dose_sem, a2a_send, a2a_recv, fwd_send, fwd_recv, pair_send, pair_recv,
    back_send, back_recv, ext_send,
):
    me = lax.axis_index("genes")
    core = lax.axis_index("samples")
    other = 1 - core
    rows, samp = dose.shape
    phen = slots + 1
    width = rows // 2
    half = SPILL // 2
    intron_rows = slots * genes
    all_rows = phen * genes
    blk = counts_ref.shape[2]
    count = float(2 * samp)
    shift = n // 2

    dose_copy = pltpu.make_async_copy(dose_hbm, dose, dose_sem)
    dose_copy.start()

    barrier = pltpu.get_barrier_semaphore()

    def greet(k, carry):
        there = lax.rem(me + k, n)
        pl.semaphore_signal(
            barrier, inc=1, device_id={"genes": there, "samples": core}, device_id_type=MESH
        )
        pl.semaphore_signal(
            barrier, inc=1, device_id={"genes": there, "samples": other}, device_id_type=MESH
        )
        return carry

    lax.fori_loop(1, n, greet, 0)
    pl.semaphore_signal(barrier, inc=1, device_id={"samples": other}, device_id_type=MESH)

    def a2a(owner, source):
        return pltpu.make_async_remote_copy(
            src_ref=sendbuf.at[owner], dst_ref=recv.at[source],
            send_sem=a2a_send.at[owner], recv_sem=a2a_recv.at[source],
            device_id={"genes": owner}, device_id_type=MESH,
        )

    slot_at = lax.broadcasted_iota(jnp.int32, ids.shape, 1)
    end = jnp.zeros((ids.shape[0], 1), jnp.int32)
    cluster_of = jnp.zeros(ids.shape, jnp.int32)
    for c in range(sizes_ref.shape[1]):
        end = end + sizes_ref[:, c : c + 1]
        cluster_of = cluster_of + (end <= slot_at).astype(jnp.int32)
    ids[...] = cluster_of
    clusters = sizes_ref.shape[1]
    cluster_row = lax.broadcasted_iota(jnp.int32, (clusters, slots), 0)
    on_diagonal = lax.broadcasted_iota(jnp.int32, (slots, slots), 0) == lax.broadcasted_iota(
        jnp.int32, (slots, slots), 1
    )

    def make_block(owner):
        for g in range(genes):
            gene = owner * genes + g
            cnt = counts_ref[block_ref[gene]]
            valid = valid_ref[pl.ds(gene, 1), :].astype(jnp.float32)
            member = (cluster_row == ids[pl.ds(gene, 1), :]).astype(jnp.float32)
            same = lax.dot_general(
                member.astype(jnp.bfloat16), (member * valid).astype(jnp.bfloat16),
                (((0,), (0,)), ((), ())), preferred_element_type=jnp.float32,
            ).astype(jnp.bfloat16)
            keep = jnp.where(on_diagonal, valid, 0.0).astype(jnp.bfloat16)
            total = jnp.dot(same, cnt, preferred_element_type=jnp.float32)
            live = jnp.dot(keep, cnt, preferred_element_type=jnp.float32)
            ratio = live / jnp.maximum(total, 1.0)
            stage[pl.ds(g, slots, stride=genes), :] = ratio
        sendbuf[owner] = stage[...].astype(jnp.bfloat16)

    def side(index):
        return index * 2 // n

    def relayed(source, owner):
        return jnp.logical_and(side(source) != side(owner), side(owner) == side(owner + 1))

    def ext(owner):
        return pltpu.make_async_remote_copy(
            src_ref=sendbuf.at[owner], dst_ref=halo.at[me],
            send_sem=ext_send.at[owner], recv_sem=fwd_recv.at[me],
            device_id={"genes": lax.rem(owner + 1, n)}, device_id_type=MESH,
        )

    def extends(owner):
        far = jnp.logical_and(owner != n - 1, owner + 1 != me)
        return jnp.logical_and(far, jnp.logical_not(relayed(me, owner)))

    def send_block(owner):
        @pl.when(owner != me)
        def _():
            a2a(owner, me).start()

        @pl.when(extends(owner))
        def _():
            ext(owner).start()

    make_block(lax.rem(me + shift, n))
    pl.semaphore_wait(barrier, 2 * n - 1)

    def ratio_step(k, carry):
        make_block(lax.rem(me + shift + k, n))

        send_block(lax.rem(me + shift + k - 1, n))
        return carry

    lax.fori_loop(1, n, ratio_step, 0)
    send_block(lax.rem(me + shift + n - 1, n))

    dose_copy.wait()
    dstat[:, rows:] = jnp.zeros((16, SPILL), jnp.float32)
    ones = jnp.ones((8, LANE), jnp.float32)
    chunk = 256

    def dose_stat(k, carry):
        at = pl.multiple_of(k * chunk, chunk)
        value = dose[pl.ds(at, chunk), :].astype(jnp.float32)
        dims = (((1,), (1,)), ((), ()))
        for slot, part in ((0, value), (8, value * value)):
            dstat[slot : slot + 8, pl.ds(at, chunk)] = lax.dot_general(
                ones, lane_tiles_sum(part), dims, precision=lax.Precision.HIGHEST,
                preferred_element_type=jnp.float32,
            )
        return carry

    lax.fori_loop(0, rows // chunk, dose_stat, 0)

    def pair(k, src, dst):
        return pltpu.make_async_remote_copy(
            src_ref=src, dst_ref=dst, send_sem=pair_send.at[k], recv_sem=pair_recv.at[k],
            device_id={"samples": other}, device_id_type=MESH,
        )

    def fwd(src, dst, k):
        return pltpu.make_async_remote_copy(
            src_ref=src, dst_ref=dst, send_sem=fwd_send.at[k], recv_sem=fwd_recv.at[k],
            device_id={"genes": lax.rem(me + 1, n)}, device_id_type=MESH,
        )

    has_next = me < n - 1
    has_prev = me > 0

    @pl.when(has_next)
    def _():
        fwd(expr_ref, halo_expr, n).start()

    def relay(k, carry):
        source = lax.rem(me + 2 * n - shift - k, n)

        @pl.when(k != n - shift)
        def _():
            a2a(source, source).wait_recv()

            @pl.when(jnp.logical_and(has_next, relayed(source, me)))
            def _():
                fwd(recv.at[source], halo.at[source], source).start()

        return carry

    dstat_pair = pair(0, dstat, dstat_in)
    dstat_pair.start()
    lax.fori_loop(0, n, relay, 0)
    recv[me] = sendbuf[me]

    def pack(blocks, expr_rows, target, stat):
        for i in range(n):
            target[:intron_rows, i * blk : (i + 1) * blk] = blocks[i]
        target[intron_rows:, :] = expr_rows[...]
        value = target[...].astype(jnp.float32)
        stat[0] = lane_tiles_sum(value)
        stat[1] = lane_tiles_sum(value * value)

    dims = (((1,), (1,)), ((), ()))
    lane_gene = lax.broadcasted_iota(jnp.int32, (genes, LANE), 0)
    starts = jnp.zeros((genes, LANE), jnp.int32)
    for g in range(genes):
        starts = jnp.where(lane_gene == g, starts_ref[g], starts)
    steps = SPILL // LANE
    at_step = [starts == s * LANE for s in range(steps)]

    def windows(source, row, base):
        tiles = []
        for t in range((width + SPILL) // LANE):
            at = pl.multiple_of(base + t * LANE, LANE)
            tiles.append(source[pl.ds(row, genes), pl.ds(at, LANE)])
        picked = []
        for t in range(width // LANE):
            tile = tiles[t + steps]
            for s in range(steps):
                tile = jnp.where(at_step[s], tiles[t + s], tile)
            picked.append(tile)
        return picked

    def scales(stat, stat_in, row):
        total = jnp.sum(stat[0, pl.ds(row, genes), :] + stat_in[0, pl.ds(row, genes), :], axis=1, keepdims=True)
        square = jnp.sum(stat[1, pl.ds(row, genes), :] + stat_in[1, pl.ds(row, genes), :], axis=1, keepdims=True)
        return total / count, lax.rsqrt(jnp.maximum(square - total * total / count, 1.0))

    def dose_scale(total, square):
        return lax.rsqrt(jnp.maximum(square - total * total / count, 1.0))

    hstat_pair = pair(3, hstat, hstat_in)
    hprod_pair = pair(4, hprod.at[other], hprod_in)
    back = pltpu.make_async_remote_copy(
        src_ref=hres, dst_ref=hres_in.at[core], send_sem=back_send, recv_sem=back_recv.at[core],
        device_id={"genes": lax.rem(me + n - 1, n), "samples": 1}, device_id_type=MESH,
    )

    @pl.when(has_prev)
    def _():
        fwd(expr_ref, halo_expr, n).wait_recv()

        def arrive(k, carry):
            @pl.when(k != me)
            def _():
                fwd(recv.at[k], halo.at[k], k).wait_recv()

            return carry

        lax.fori_loop(0, n, arrive, 0)
        halo[me] = sendbuf[lax.rem(me + n - 1, n)]
        pack(halo, halo_expr, hpheno, hstat)

        def halo_dot(k, carry):
            at = pl.multiple_of(k * half, half)
            hprod[k] = lax.dot_general(
                hpheno[...], dose[pl.ds(at, half), :], dims, preferred_element_type=jnp.float32
            )
            return carry

        lax.fori_loop(0, 2, halo_dot, 0)
        hstat_pair.start()
        hprod_pair.start()

    pack(recv, expr_ref, pheno, pstat)
    pstat_pair = pair(1, pstat, pstat_in)

    prod[:, rows:] = jnp.zeros((all_rows, SPILL), jnp.float32)

    def own_dot(k, carry):
        at = pl.multiple_of(k * chunk, chunk)
        prod[:, pl.ds(at, chunk)] = lax.dot_general(
            pheno[...], dose[pl.ds(at, chunk), :], dims, preferred_element_type=jnp.float32
        )
        return carry

    lax.fori_loop(0, rows // chunk, own_dot, 0)
    pstat_pair.start()

    dstat_pair.wait_recv()
    dstat_pair.wait_send()
    dstat[...] = dstat[...] + dstat_in[...]

    @pl.when(has_prev)
    def _():
        hstat_pair.wait_recv()
        hprod_pair.wait_recv()
        at = pl.multiple_of(core * half, half)
        sums = dstat[0:8, pl.ds(at, half)]
        scale = dose_scale(sums, dstat[8:16, pl.ds(at, half)])

        def halo_out(p, carry):
            row = pl.multiple_of(p * genes, genes)
            mean, inv = scales(hstat, hstat_in, row)
            cross = hprod[core, pl.ds(row, genes), :] + hprod_in[pl.ds(row, genes), :]
            hres[p] = ((cross - sums * mean) * scale * inv).astype(jnp.bfloat16)
            return carry

        lax.fori_loop(0, phen, halo_out, 0)
        back.start()

    def select_out(p, carry):
        row = pl.multiple_of(p * genes, genes)
        for t, tile in enumerate(windows(prod, row, other * width)):
            sel_out[pl.ds(row, genes), t * LANE : (t + 1) * LANE] = tile
        return carry

    lax.fori_loop(0, phen, select_out, 0)
    sel_pair = pair(2, sel_out, sel_in)
    sel_pair.start()

    pstat_pair.wait_recv()
    sel_pair.wait_recv()
    win_sum = windows(dstat, 0, core * width)
    win_square = windows(dstat, 8, core * width)
    for t in range(width // LANE):
        cols = slice(t * LANE, (t + 1) * LANE)
        win[0:8, cols] = win_sum[t]
        win[8:16, cols] = dose_scale(win_sum[t], win_square[t])

    def own_out(p, carry):
        row = pl.multiple_of(p * genes, genes)
        mean, inv = scales(pstat, pstat_in, row)
        for t, tile in enumerate(windows(prod, row, core * width)):
            cols = slice(t * LANE, (t + 1) * LANE)
            cross = tile + sel_in[pl.ds(row, genes), cols]
            own_res[pl.ds(row, genes), cols] = (cross - win[0:8, cols] * mean) * win[8:16, cols] * inv
        return carry

    lax.fori_loop(0, phen, own_out, 0)
    takes_halo = jnp.logical_and(has_next, core == 1)

    @pl.when(takes_halo)
    def _():
        for side in range(2):
            pltpu.make_async_remote_copy(
                src_ref=hres, dst_ref=hres_in.at[side], send_sem=back_send,
                recv_sem=back_recv.at[side],
                device_id={"genes": lax.rem(me + n - 1, n), "samples": 1}, device_id_type=MESH,
            ).wait_recv()
        halo_full[:, :width] = jnp.zeros((all_rows, width), jnp.float32)

        def widen(p, carry):
            row = pl.multiple_of(p * genes, genes)
            for side in range(2):
                halo_full[pl.ds(row, genes), width + side * half : width + (side + 1) * half] = (
                    hres_in[side, p].astype(jnp.float32)
                )
            return carry

        lax.fori_loop(0, phen, widen, 0)

        def add_halo(p, carry):
            row = pl.multiple_of(p * genes, genes)
            for t, tile in enumerate(windows(halo_full, row, 0)):
                cols = slice(t * LANE, (t + 1) * LANE)
                out_ref[lax.rem(p + 1, phen), :, cols] = (
                    own_res[pl.ds(row, genes), cols] + tile
                ).astype(jnp.bfloat16)
            return carry

        lax.fori_loop(0, phen, add_halo, 0)

    @pl.when(jnp.logical_not(takes_halo))
    def _():
        def plain(p, carry):
            row = pl.multiple_of(p * genes, genes)
            out_ref[lax.rem(p + 1, phen)] = own_res[pl.ds(row, genes), :].astype(jnp.bfloat16)
            return carry

        lax.fori_loop(0, phen, plain, 0)

    def drain(k, carry):
        a2a(lax.rem(me + k, n), me).wait_send()
        return carry

    lax.fori_loop(1, n, drain, 0)

    def drain_ext(k, carry):
        @pl.when(extends(k))
        def _():
            ext(k).wait_send()

        return carry

    lax.fori_loop(0, n, drain_ext, 0)
    pstat_pair.wait_send()
    sel_pair.wait_send()

    @pl.when(has_next)
    def _():
        fwd(expr_ref, halo_expr, n).wait_send()

        def drain_fwd(k, carry):
            @pl.when(relayed(k, me))
            def _():
                fwd(recv.at[k], halo.at[k], k).wait_send()

            return carry

        lax.fori_loop(0, n, drain_fwd, 0)

    @pl.when(has_prev)
    def _():
        hstat_pair.wait_send()
        hprod_pair.wait_send()
        back.wait_send()


def shards(dosage, expression, intron_counts, cluster_sizes, valid_mask, gene_block, window_start):
    n = lax.axis_size("genes")
    rows, samp = dosage.shape
    genes = expression.shape[0]
    slots = valid_mask.shape[1]
    blk = intron_counts.shape[0]
    phen = slots + 1
    all_rows = phen * genes
    width = rows // 2
    half = SPILL // 2
    counts_t = intron_counts.T.reshape(n * genes, slots, blk)
    vmem = pl.BlockSpec(memory_space=pltpu.VMEM)
    smem = pl.BlockSpec(memory_space=pltpu.SMEM)
    f32, bf16 = jnp.float32, jnp.bfloat16
    dma = pltpu.SemaphoreType.DMA
    result = pl.pallas_call(
        functools.partial(kernel, n, genes, slots),
        out_shape=jax.ShapeDtypeStruct((phen, genes, width), bf16),
        in_specs=[smem, smem, vmem, vmem, vmem, vmem, pl.BlockSpec(memory_space=pl.ANY)],
        out_specs=vmem,
        scratch_shapes=[
            pltpu.VMEM((rows, samp), bf16),
            pltpu.VMEM((n * genes, slots), jnp.int32),
            pltpu.VMEM((slots * genes, blk), f32),
            pltpu.VMEM((n, slots * genes, blk), bf16),
            pltpu.VMEM((n, slots * genes, blk), bf16),
            pltpu.VMEM((n, slots * genes, blk), bf16),
            pltpu.VMEM((genes, samp), bf16),
            pltpu.VMEM((all_rows, samp), bf16),
            pltpu.VMEM((all_rows, samp), bf16),
            pltpu.VMEM((all_rows, rows + SPILL), f32),
            pltpu.VMEM((2, all_rows, half), f32),
            pltpu.VMEM((all_rows, half), f32),
            pltpu.VMEM((all_rows, width), f32),
            pltpu.VMEM((all_rows, width), f32),
            pltpu.VMEM((all_rows, width), f32),
            pltpu.VMEM((all_rows, width + SPILL), f32),
            pltpu.VMEM((16, rows + SPILL), f32),
            pltpu.VMEM((16, rows + SPILL), f32),
            pltpu.VMEM((2, all_rows, LANE), f32),
            pltpu.VMEM((2, all_rows, LANE), f32),
            pltpu.VMEM((2, all_rows, LANE), f32),
            pltpu.VMEM((2, all_rows, LANE), f32),
            pltpu.VMEM((phen, genes, half), bf16),
            pltpu.VMEM((2, phen, genes, half), bf16),
            pltpu.VMEM((16, width), f32),
            dma, dma((n,)), dma((n,)), dma((n + 1,)), dma((n + 1,)), dma((5,)), dma((5,)),
            dma, dma((2,)), dma((n,)),
        ],
        compiler_params=pltpu.CompilerParams(
            collective_id=0, has_side_effects=True, vmem_limit_bytes=62 * 1024 * 1024
        ),
    )(window_start, gene_block, counts_t, cluster_sizes, valid_mask, expression, dosage)
    return jnp.transpose(result, (1, 0, 2))


def solution(mesh):
    in_specs = (
        P(("parts", "genes"), "samples"),
        P(("parts", "genes"), "samples"),
        P(("parts", "samples", "genes"), None),
        P("parts", None),
        P("parts", None),
        P("parts"),
        P(("parts", "genes")),
    )
    out_specs = P(("parts", "genes"), None, "samples")
    return jax.shard_map(shards, mesh=mesh, in_specs=in_specs, out_specs=out_specs, check_vma=False)
```

```python
import functools
import math

import jax
import jax.numpy as jnp
from jax import lax
from jax.experimental import pallas as pl
from jax.experimental.pallas import tpu as pltpu
from jax.sharding import PartitionSpec as P

LANE = 128
SPILL = 1024
MESH = pl.DeviceIdType.MESH


def lane_tiles_sum(value):
    total = value[:, :LANE]
    for t in range(1, value.shape[1] // LANE):
        total = total + value[:, t * LANE : (t + 1) * LANE]
    return total


def kernel(
    n, genes, slots, starts_ref, block_ref, counts_ref, sizes_ref, valid_ref, expr_ref, dose_hbm, out_ref,
    dose, ids, counts_t, stage, sendbuf, recv, halo, halo_expr, pheno, hpheno, prod, hprod, hprod_in,
    sel_out, sel_in, own_res, halo_full, dstat, dstat_in, pstat, pstat_in, hstat, hstat_in,
    hres, hres_in, win, dose_sem, a2a_send, a2a_recv, fwd_send, fwd_recv, pair_send, pair_recv,
    back_send, back_recv, ext_send,
):
    me = lax.axis_index("genes")
    core = lax.axis_index("samples")
    other = 1 - core
    rows, samp = dose.shape
    phen = slots + 1
    width = rows // 2
    half = SPILL // 2
    intron_rows = slots * genes
    all_rows = phen * genes
    blk = counts_ref.shape[0]
    count = float(2 * samp)
    shift = n // 2

    dose_copy = pltpu.make_async_copy(dose_hbm, dose, dose_sem)
    dose_copy.start()

    barrier = pltpu.get_barrier_semaphore()

    def greet(k, carry):
        there = lax.rem(me + k, n)
        pl.semaphore_signal(
            barrier, inc=1, device_id={"genes": there, "samples": core}, device_id_type=MESH
        )
        pl.semaphore_signal(
            barrier, inc=1, device_id={"genes": there, "samples": other}, device_id_type=MESH
        )
        return carry

    lax.fori_loop(1, n, greet, 0)
    pl.semaphore_signal(barrier, inc=1, device_id={"samples": other}, device_id_type=MESH)

    def a2a(owner, source):
        return pltpu.make_async_remote_copy(
            src_ref=sendbuf.at[owner], dst_ref=recv.at[source],
            send_sem=a2a_send.at[owner], recv_sem=a2a_recv.at[source],
            device_id={"genes": owner}, device_id_type=MESH,
        )

    clusters = sizes_ref.shape[0]
    slot_at = lax.broadcasted_iota(jnp.int32, valid_ref.shape, 0)
    end = jnp.zeros((1, valid_ref.shape[1]), jnp.int32)
    cluster_of = jnp.zeros(valid_ref.shape, jnp.int32)
    for c in range(clusters):
        end = end + sizes_ref[c : c + 1, :]
        cluster_of = cluster_of + (end <= slot_at).astype(jnp.int32)
    ids[0] = cluster_of.astype(jnp.float32).T
    ids[1] = valid_ref[...].astype(jnp.float32).T
    group = math.lcm(slots, LANE)
    per = group // slots

    def turn(k, carry):
        at = pl.multiple_of(k * group, group)
        piece = counts_ref[:, pl.ds(at, group)].astype(jnp.float32)
        counts_t[pl.ds(k * per, per)] = piece.T.reshape(per, slots, blk)
        return carry

    lax.fori_loop(0, counts_ref.shape[1] // group, turn, 0)
    cluster_row = lax.broadcasted_iota(jnp.int32, (clusters, slots), 0)
    on_diagonal = lax.broadcasted_iota(jnp.int32, (slots, slots), 0) == lax.broadcasted_iota(
        jnp.int32, (slots, slots), 1
    )

    def make_block(owner):
        for g in range(genes):
            gene = owner * genes + g
            cnt = counts_t[block_ref[gene]].astype(jnp.bfloat16)
            valid = ids[1, pl.ds(gene, 1), :]
            member = (cluster_row == ids[0, pl.ds(gene, 1), :].astype(jnp.int32)).astype(jnp.float32)
            same = lax.dot_general(
                member.astype(jnp.bfloat16), (member * valid).astype(jnp.bfloat16),
                (((0,), (0,)), ((), ())), preferred_element_type=jnp.float32,
            ).astype(jnp.bfloat16)
            keep = jnp.where(on_diagonal, valid, 0.0).astype(jnp.bfloat16)
            total = jnp.dot(same, cnt, preferred_element_type=jnp.float32)
            live = jnp.dot(keep, cnt, preferred_element_type=jnp.float32)
            ratio = live / jnp.maximum(total, 1.0)
            stage[pl.ds(g, slots, stride=genes), :] = ratio
        sendbuf[owner] = stage[...].astype(jnp.bfloat16)

    def side(index):
        return index * 2 // n

    def relayed(source, owner):
        return jnp.logical_and(side(source) != side(owner), side(owner) == side(owner + 1))

    def ext(owner):
        return pltpu.make_async_remote_copy(
            src_ref=sendbuf.at[owner], dst_ref=halo.at[me],
            send_sem=ext_send.at[owner], recv_sem=fwd_recv.at[me],
            device_id={"genes": lax.rem(owner + 1, n)}, device_id_type=MESH,
        )

    def extends(owner):
        far = jnp.logical_and(owner != n - 1, owner + 1 != me)
        return jnp.logical_and(far, jnp.logical_not(relayed(me, owner)))

    def early(source, owner):
        return jnp.logical_and(owner != n - 1, relayed(source, owner))

    def send_block(owner):
        @pl.when(extends(owner))
        def _():
            ext(owner).start()

        @pl.when(early(me, owner))
        def _():
            a2a(owner, me).start()

    make_block(lax.rem(me + shift, n))
    pl.semaphore_wait(barrier, 2 * n - 1)

    def ratio_step(k, carry):
        make_block(lax.rem(me + shift + k, n))

        send_block(lax.rem(me + shift + k - 1, n))
        return carry

    lax.fori_loop(1, n, ratio_step, 0)
    send_block(lax.rem(me + shift + n - 1, n))

    def late_step(k, carry):
        owner = lax.rem(me + k, n)

        @pl.when(jnp.logical_not(early(me, owner)))
        def _():
            a2a(owner, me).start()

        return carry

    lax.fori_loop(1, n, late_step, 0)

    dose_copy.wait()
    dstat[:, rows:] = jnp.zeros((16, SPILL), jnp.float32)
    ones = jnp.ones((8, LANE), jnp.float32)
    chunk = 256

    def dose_stat(k, carry):
        at = pl.multiple_of(k * chunk, chunk)
        value = dose[pl.ds(at, chunk), :].astype(jnp.float32)
        dims = (((1,), (1,)), ((), ()))
        for slot, part in ((0, value), (8, value * value)):
            dstat[slot : slot + 8, pl.ds(at, chunk)] = lax.dot_general(
                ones, lane_tiles_sum(part), dims, precision=lax.Precision.HIGHEST,
                preferred_element_type=jnp.float32,
            )
        return carry

    lax.fori_loop(0, rows // chunk, dose_stat, 0)

    def pair(k, src, dst):
        return pltpu.make_async_remote_copy(
            src_ref=src, dst_ref=dst, send_sem=pair_send.at[k], recv_sem=pair_recv.at[k],
            device_id={"samples": other}, device_id_type=MESH,
        )

    def fwd(src, dst, k):
        return pltpu.make_async_remote_copy(
            src_ref=src, dst_ref=dst, send_sem=fwd_send.at[k], recv_sem=fwd_recv.at[k],
            device_id={"genes": lax.rem(me + 1, n)}, device_id_type=MESH,
        )

    has_next = me < n - 1
    has_prev = me > 0

    @pl.when(has_next)
    def _():
        fwd(expr_ref, halo_expr, n).start()

    def relay(k, carry):
        source = lax.rem(me + 2 * n - shift - k, n)

        @pl.when(early(source, me))
        def _():
            a2a(source, source).wait_recv()
            fwd(recv.at[source], halo.at[source], source).start()

        return carry

    def own_arrive(k, carry):
        source = lax.rem(me + k, n)

        @pl.when(jnp.logical_not(early(source, me)))
        def _():
            a2a(source, source).wait_recv()

        return carry

    dstat_pair = pair(0, dstat, dstat_in)
    dstat_pair.start()
    lax.fori_loop(0, n, relay, 0)

    def pack(blocks, expr_rows, target, stat):
        for i in range(n):
            target[:intron_rows, i * blk : (i + 1) * blk] = blocks[i]
        target[intron_rows:, :] = expr_rows[...]
        value = target[...].astype(jnp.float32)
        stat[0] = lane_tiles_sum(value)
        stat[1] = lane_tiles_sum(value * value)

    dims = (((1,), (1,)), ((), ()))
    lane_gene = lax.broadcasted_iota(jnp.int32, (genes, LANE), 0)
    starts = jnp.zeros((genes, LANE), jnp.int32)
    for g in range(genes):
        starts = jnp.where(lane_gene == g, starts_ref[g], starts)
    steps = SPILL // LANE
    at_step = [starts == s * LANE for s in range(steps)]

    def windows(source, row, base):
        tiles = []
        for t in range((width + SPILL) // LANE):
            at = pl.multiple_of(base + t * LANE, LANE)
            tiles.append(source[pl.ds(row, genes), pl.ds(at, LANE)])
        picked = []
        for t in range(width // LANE):
            tile = tiles[t + steps]
            for s in range(steps):
                tile = jnp.where(at_step[s], tiles[t + s], tile)
            picked.append(tile)
        return picked

    def scales(stat, stat_in, row):
        total = jnp.sum(stat[0, pl.ds(row, genes), :] + stat_in[0, pl.ds(row, genes), :], axis=1, keepdims=True)
        square = jnp.sum(stat[1, pl.ds(row, genes), :] + stat_in[1, pl.ds(row, genes), :], axis=1, keepdims=True)
        return total / count, lax.rsqrt(jnp.maximum(square - total * total / count, 1.0))

    def dose_scale(total, square):
        return lax.rsqrt(jnp.maximum(square - total * total / count, 1.0))

    hstat_pair = pair(3, hstat, hstat_in)
    hprod_pair = pair(4, hprod.at[other], hprod_in)
    back = pltpu.make_async_remote_copy(
        src_ref=hres, dst_ref=hres_in.at[core], send_sem=back_send, recv_sem=back_recv.at[core],
        device_id={"genes": lax.rem(me + n - 1, n), "samples": 1}, device_id_type=MESH,
    )

    @pl.when(has_prev)
    def _():
        fwd(expr_ref, halo_expr, n).wait_recv()

        def arrive(k, carry):
            @pl.when(k != me)
            def _():
                fwd(recv.at[k], halo.at[k], k).wait_recv()

            return carry

        lax.fori_loop(0, n, arrive, 0)
        halo[me] = sendbuf[lax.rem(me + n - 1, n)]
        pack(halo, halo_expr, hpheno, hstat)

        def halo_dot(k, carry):
            at = pl.multiple_of(k * half, half)
            hprod[k] = lax.dot_general(
                hpheno[...], dose[pl.ds(at, half), :], dims, preferred_element_type=jnp.float32
            )
            return carry

        lax.fori_loop(0, 2, halo_dot, 0)
        hstat_pair.start()
        hprod_pair.start()

    dstat_pair.wait_recv()
    dstat_pair.wait_send()
    dstat[...] = dstat[...] + dstat_in[...]

    @pl.when(has_prev)
    def _():
        hstat_pair.wait_recv()
        hprod_pair.wait_recv()
        at = pl.multiple_of(core * half, half)
        sums = dstat[0:8, pl.ds(at, half)]
        scale = dose_scale(sums, dstat[8:16, pl.ds(at, half)])

        def halo_out(p, carry):
            row = pl.multiple_of(p * genes, genes)
            mean, inv = scales(hstat, hstat_in, row)
            cross = hprod[core, pl.ds(row, genes), :] + hprod_in[pl.ds(row, genes), :]
            hres[p] = ((cross - sums * mean) * scale * inv).astype(jnp.bfloat16)
            return carry

        lax.fori_loop(0, phen, halo_out, 0)
        back.start()

    lax.fori_loop(1, n, own_arrive, 0)
    recv[me] = sendbuf[me]
    pack(recv, expr_ref, pheno, pstat)
    pstat_pair = pair(1, pstat, pstat_in)

    prod[:, rows:] = jnp.zeros((all_rows, SPILL), jnp.float32)

    def own_dot(k, carry):
        at = pl.multiple_of(k * chunk, chunk)
        prod[:, pl.ds(at, chunk)] = lax.dot_general(
            pheno[...], dose[pl.ds(at, chunk), :], dims, preferred_element_type=jnp.float32
        )
        return carry

    lax.fori_loop(0, rows // chunk, own_dot, 0)
    pstat_pair.start()

    def select_out(p, carry):
        row = pl.multiple_of(p * genes, genes)
        for t, tile in enumerate(windows(prod, row, other * width)):
            sel_out[pl.ds(row, genes), t * LANE : (t + 1) * LANE] = tile
        return carry

    lax.fori_loop(0, phen, select_out, 0)
    sel_pair = pair(2, sel_out, sel_in)
    sel_pair.start()

    pstat_pair.wait_recv()
    sel_pair.wait_recv()
    win_sum = windows(dstat, 0, core * width)
    win_square = windows(dstat, 8, core * width)
    for t in range(width // LANE):
        cols = slice(t * LANE, (t + 1) * LANE)
        win[0:8, cols] = win_sum[t]
        win[8:16, cols] = dose_scale(win_sum[t], win_square[t])

    def own_out(p, carry):
        row = pl.multiple_of(p * genes, genes)
        mean, inv = scales(pstat, pstat_in, row)
        for t, tile in enumerate(windows(prod, row, core * width)):
            cols = slice(t * LANE, (t + 1) * LANE)
            cross = tile + sel_in[pl.ds(row, genes), cols]
            own_res[pl.ds(row, genes), cols] = (cross - win[0:8, cols] * mean) * win[8:16, cols] * inv
        return carry

    lax.fori_loop(0, phen, own_out, 0)
    takes_halo = jnp.logical_and(has_next, core == 1)

    @pl.when(takes_halo)
    def _():
        for side in range(2):
            pltpu.make_async_remote_copy(
                src_ref=hres, dst_ref=hres_in.at[side], send_sem=back_send,
                recv_sem=back_recv.at[side],
                device_id={"genes": lax.rem(me + n - 1, n), "samples": 1}, device_id_type=MESH,
            ).wait_recv()
        halo_full[:, :width] = jnp.zeros((all_rows, width), jnp.float32)

        def widen(p, carry):
            row = pl.multiple_of(p * genes, genes)
            for side in range(2):
                halo_full[pl.ds(row, genes), width + side * half : width + (side + 1) * half] = (
                    hres_in[side, p].astype(jnp.float32)
                )
            return carry

        lax.fori_loop(0, phen, widen, 0)

        def add_halo(p, carry):
            row = pl.multiple_of(p * genes, genes)
            for t, tile in enumerate(windows(halo_full, row, 0)):
                cols = slice(t * LANE, (t + 1) * LANE)
                out_ref[lax.rem(p + 1, phen), :, cols] = (
                    own_res[pl.ds(row, genes), cols] + tile
                ).astype(jnp.bfloat16)
            return carry

        lax.fori_loop(0, phen, add_halo, 0)

    @pl.when(jnp.logical_not(takes_halo))
    def _():
        def plain(p, carry):
            row = pl.multiple_of(p * genes, genes)
            out_ref[lax.rem(p + 1, phen)] = own_res[pl.ds(row, genes), :].astype(jnp.bfloat16)
            return carry

        lax.fori_loop(0, phen, plain, 0)

    def drain(k, carry):
        a2a(lax.rem(me + k, n), me).wait_send()
        return carry

    lax.fori_loop(1, n, drain, 0)

    def drain_ext(k, carry):
        @pl.when(extends(k))
        def _():
            ext(k).wait_send()

        return carry

    lax.fori_loop(0, n, drain_ext, 0)
    pstat_pair.wait_send()
    sel_pair.wait_send()

    @pl.when(has_next)
    def _():
        fwd(expr_ref, halo_expr, n).wait_send()

        def drain_fwd(k, carry):
            @pl.when(relayed(k, me))
            def _():
                fwd(recv.at[k], halo.at[k], k).wait_send()

            return carry

        lax.fori_loop(0, n, drain_fwd, 0)

    @pl.when(has_prev)
    def _():
        hstat_pair.wait_send()
        hprod_pair.wait_send()
        back.wait_send()


def shards(dosage, expression, intron_counts, cluster_sizes, valid_mask, gene_block, window_start):
    n = lax.axis_size("genes")
    rows, samp = dosage.shape
    genes = expression.shape[0]
    slots = valid_mask.shape[1]
    blk = intron_counts.shape[0]
    phen = slots + 1
    all_rows = phen * genes
    width = rows // 2
    half = SPILL // 2
    vmem = pl.BlockSpec(memory_space=pltpu.VMEM)
    smem = pl.BlockSpec(memory_space=pltpu.SMEM)
    f32, bf16 = jnp.float32, jnp.bfloat16
    dma = pltpu.SemaphoreType.DMA
    result = pl.pallas_call(
        functools.partial(kernel, n, genes, slots),
        out_shape=jax.ShapeDtypeStruct((phen, genes, width), bf16),
        in_specs=[smem, smem, vmem, vmem, vmem, vmem, pl.BlockSpec(memory_space=pl.ANY)],
        out_specs=vmem,
        scratch_shapes=[
            pltpu.VMEM((rows, samp), bf16),
            pltpu.VMEM((2, n * genes, slots), f32),
            pltpu.VMEM((n * genes, slots, blk), f32),
            pltpu.VMEM((slots * genes, blk), f32),
            pltpu.VMEM((n, slots * genes, blk), bf16),
            pltpu.VMEM((n, slots * genes, blk), bf16),
            pltpu.VMEM((n, slots * genes, blk), bf16),
            pltpu.VMEM((genes, samp), bf16),
            pltpu.VMEM((all_rows, samp), bf16),
            pltpu.VMEM((all_rows, samp), bf16),
            pltpu.VMEM((all_rows, rows + SPILL), f32),
            pltpu.VMEM((2, all_rows, half), f32),
            pltpu.VMEM((all_rows, half), f32),
            pltpu.VMEM((all_rows, width), f32),
            pltpu.VMEM((all_rows, width), f32),
            pltpu.VMEM((all_rows, width), f32),
            pltpu.VMEM((all_rows, width + SPILL), f32),
            pltpu.VMEM((16, rows + SPILL), f32),
            pltpu.VMEM((16, rows + SPILL), f32),
            pltpu.VMEM((2, all_rows, LANE), f32),
            pltpu.VMEM((2, all_rows, LANE), f32),
            pltpu.VMEM((2, all_rows, LANE), f32),
            pltpu.VMEM((2, all_rows, LANE), f32),
            pltpu.VMEM((phen, genes, half), bf16),
            pltpu.VMEM((2, phen, genes, half), bf16),
            pltpu.VMEM((16, width), f32),
            dma, dma((n,)), dma((n,)), dma((n + 1,)), dma((n + 1,)), dma((5,)), dma((5,)),
            dma, dma((2,)), dma((n,)),
        ],
        compiler_params=pltpu.CompilerParams(
            collective_id=0, has_side_effects=True, vmem_limit_bytes=62 * 1024 * 1024
        ),
    )(window_start, gene_block, intron_counts, cluster_sizes.T, valid_mask.T, expression, dosage)
    return jnp.transpose(result, (1, 0, 2))


def solution(mesh):
    in_specs = (
        P(("parts", "genes"), "samples"),
        P(("parts", "genes"), "samples"),
        P(("parts", "samples", "genes"), None),
        P("parts", None),
        P("parts", None),
        P("parts"),
        P(("parts", "genes")),
    )
    out_specs = P(("parts", "genes"), None, "samples")
    return jax.shard_map(shards, mesh=mesh, in_specs=in_specs, out_specs=out_specs, check_vma=False)
```

```python
import functools
import math

import jax
import jax.numpy as jnp
from jax import lax
from jax.experimental import pallas as pl
from jax.experimental.pallas import tpu as pltpu
from jax.sharding import PartitionSpec as P

LANE = 128
SPILL = 1024
MESH = pl.DeviceIdType.MESH


def lane_tiles_sum(value):
    total = value[:, :LANE]
    for t in range(1, value.shape[1] // LANE):
        total = total + value[:, t * LANE : (t + 1) * LANE]
    return total


def kernel(
    n, genes, slots, starts_ref, block_ref, counts_ref, sizes_ref, valid_ref, expr_ref, dose_hbm, out_ref,
    dose, ids, counts_t, stage, sendbuf, recv, halo, halo_expr, pheno, hpheno, prod, hprod, hprod_in,
    sel_out, sel_in, own_res, halo_full, dstat, dstat_in, pstat, pstat_in, hstat, hstat_in,
    hres, hres_in, win, dose_sem, a2a_send, a2a_recv, fwd_send, fwd_recv, pair_send, pair_recv,
    back_send, back_recv, ext_send,
):
    me = lax.axis_index("genes")
    core = lax.axis_index("samples")
    other = 1 - core
    rows, samp = dose.shape
    phen = slots + 1
    width = rows // 2
    half = SPILL // 2
    intron_rows = slots * genes
    all_rows = phen * genes
    blk = counts_ref.shape[0]
    count = float(2 * samp)
    shift = n // 2

    dose_copy = pltpu.make_async_copy(dose_hbm, dose, dose_sem)
    dose_copy.start()

    barrier = pltpu.get_barrier_semaphore()

    def greet(k, carry):
        there = lax.rem(me + k, n)
        pl.semaphore_signal(
            barrier, inc=1, device_id={"genes": there, "samples": core}, device_id_type=MESH
        )
        pl.semaphore_signal(
            barrier, inc=1, device_id={"genes": there, "samples": other}, device_id_type=MESH
        )
        return carry

    lax.fori_loop(1, n, greet, 0)
    pl.semaphore_signal(barrier, inc=1, device_id={"samples": other}, device_id_type=MESH)

    def a2a(owner, source):
        return pltpu.make_async_remote_copy(
            src_ref=sendbuf.at[owner], dst_ref=recv.at[source],
            send_sem=a2a_send.at[owner], recv_sem=a2a_recv.at[source],
            device_id={"genes": owner}, device_id_type=MESH,
        )

    clusters = sizes_ref.shape[0]
    slot_at = lax.broadcasted_iota(jnp.int32, valid_ref.shape, 0)
    end = jnp.zeros((1, valid_ref.shape[1]), jnp.int32)
    cluster_of = jnp.zeros(valid_ref.shape, jnp.int32)
    for c in range(clusters):
        end = end + sizes_ref[c : c + 1, :]
        cluster_of = cluster_of + (end <= slot_at).astype(jnp.int32)
    ids[0] = cluster_of.astype(jnp.float32).T
    ids[1] = valid_ref[...].astype(jnp.float32).T
    group = math.lcm(slots, LANE)
    per = group // slots

    def turn(k, carry):
        at = pl.multiple_of(k * group, group)
        piece = counts_ref[:, pl.ds(at, group)].astype(jnp.float32)
        counts_t[pl.ds(k * per, per)] = piece.T.reshape(per, slots, blk)
        return carry

    lax.fori_loop(0, counts_ref.shape[1] // group, turn, 0)
    cluster_row = lax.broadcasted_iota(jnp.int32, (clusters, slots), 0)
    on_diagonal = lax.broadcasted_iota(jnp.int32, (slots, slots), 0) == lax.broadcasted_iota(
        jnp.int32, (slots, slots), 1
    )

    def make_block(owner):
        for g in range(genes):
            gene = owner * genes + g
            cnt = counts_t[block_ref[gene]].astype(jnp.bfloat16)
            valid = ids[1, pl.ds(gene, 1), :]
            member = (cluster_row == ids[0, pl.ds(gene, 1), :].astype(jnp.int32)).astype(jnp.float32)
            same = lax.dot_general(
                member.astype(jnp.bfloat16), (member * valid).astype(jnp.bfloat16),
                (((0,), (0,)), ((), ())), preferred_element_type=jnp.float32,
            ).astype(jnp.bfloat16)
            keep = jnp.where(on_diagonal, valid, 0.0).astype(jnp.bfloat16)
            total = jnp.dot(same, cnt, preferred_element_type=jnp.float32)
            live = jnp.dot(keep, cnt, preferred_element_type=jnp.float32)
            ratio = live / jnp.maximum(total, 1.0)
            stage[pl.ds(g, slots, stride=genes), :] = ratio
        sendbuf[owner] = stage[...].astype(jnp.bfloat16)

    def side(index):
        return index * 2 // n

    def relayed(source, owner):
        return jnp.logical_and(side(source) != side(owner), side(owner) == side(owner + 1))

    def ext(owner):
        return pltpu.make_async_remote_copy(
            src_ref=sendbuf.at[owner], dst_ref=halo.at[me],
            send_sem=ext_send.at[owner], recv_sem=fwd_recv.at[me],
            device_id={"genes": lax.rem(owner + 1, n)}, device_id_type=MESH,
        )

    def extends(owner):
        far = jnp.logical_and(owner != n - 1, owner + 1 != me)
        return jnp.logical_and(far, jnp.logical_not(relayed(me, owner)))

    def early(source, owner):
        return jnp.logical_and(owner != n - 1, relayed(source, owner))

    def send_block(owner):
        @pl.when(extends(owner))
        def _():
            ext(owner).start()

        @pl.when(owner != me)
        def _():
            a2a(owner, me).start()

    make_block(lax.rem(me + shift, n))
    pl.semaphore_wait(barrier, 2 * n - 1)

    def ratio_step(k, carry):
        make_block(lax.rem(me + shift + k, n))

        send_block(lax.rem(me + shift + k - 1, n))
        return carry

    lax.fori_loop(1, n, ratio_step, 0)
    send_block(lax.rem(me + shift + n - 1, n))

    dose_copy.wait()
    dstat[:, rows:] = jnp.zeros((16, SPILL), jnp.float32)
    ones = jnp.ones((8, LANE), jnp.float32)
    chunk = 256

    def dose_stat(k, carry):
        at = pl.multiple_of(k * chunk, chunk)
        value = dose[pl.ds(at, chunk), :].astype(jnp.float32)
        dims = (((1,), (1,)), ((), ()))
        for slot, part in ((0, value), (8, value * value)):
            dstat[slot : slot + 8, pl.ds(at, chunk)] = lax.dot_general(
                ones, lane_tiles_sum(part), dims, precision=lax.Precision.HIGHEST,
                preferred_element_type=jnp.float32,
            )
        return carry

    lax.fori_loop(0, rows // chunk, dose_stat, 0)

    def pair(k, src, dst):
        return pltpu.make_async_remote_copy(
            src_ref=src, dst_ref=dst, send_sem=pair_send.at[k], recv_sem=pair_recv.at[k],
            device_id={"samples": other}, device_id_type=MESH,
        )

    def fwd(src, dst, k):
        return pltpu.make_async_remote_copy(
            src_ref=src, dst_ref=dst, send_sem=fwd_send.at[k], recv_sem=fwd_recv.at[k],
            device_id={"genes": lax.rem(me + 1, n)}, device_id_type=MESH,
        )

    has_next = me < n - 1
    has_prev = me > 0

    @pl.when(has_next)
    def _():
        fwd(expr_ref, halo_expr, n).start()

    def relay(k, carry):
        source = lax.rem(me + 2 * n - shift - k, n)

        @pl.when(early(source, me))
        def _():
            a2a(source, source).wait_recv()
            fwd(recv.at[source], halo.at[source], source).start()

        return carry

    def own_arrive(k, carry):
        source = lax.rem(me + k, n)

        @pl.when(jnp.logical_not(early(source, me)))
        def _():
            a2a(source, source).wait_recv()

        return carry

    dstat_pair = pair(0, dstat, dstat_in)
    dstat_pair.start()
    lax.fori_loop(0, n, relay, 0)

    def pack(blocks, expr_rows, target, stat):
        for i in range(n):
            target[:intron_rows, i * blk : (i + 1) * blk] = blocks[i]
        target[intron_rows:, :] = expr_rows[...]
        value = target[...].astype(jnp.float32)
        stat[0] = lane_tiles_sum(value)
        stat[1] = lane_tiles_sum(value * value)

    dims = (((1,), (1,)), ((), ()))
    lane_gene = lax.broadcasted_iota(jnp.int32, (genes, LANE), 0)
    starts = jnp.zeros((genes, LANE), jnp.int32)
    for g in range(genes):
        starts = jnp.where(lane_gene == g, starts_ref[g], starts)
    steps = SPILL // LANE
    at_step = [starts == s * LANE for s in range(steps)]

    def windows(source, row, base):
        tiles = []
        for t in range((width + SPILL) // LANE):
            at = pl.multiple_of(base + t * LANE, LANE)
            tiles.append(source[pl.ds(row, genes), pl.ds(at, LANE)])
        picked = []
        for t in range(width // LANE):
            tile = tiles[t + steps]
            for s in range(steps):
                tile = jnp.where(at_step[s], tiles[t + s], tile)
            picked.append(tile)
        return picked

    def scales(stat, stat_in, row):
        total = jnp.sum(stat[0, pl.ds(row, genes), :] + stat_in[0, pl.ds(row, genes), :], axis=1, keepdims=True)
        square = jnp.sum(stat[1, pl.ds(row, genes), :] + stat_in[1, pl.ds(row, genes), :], axis=1, keepdims=True)
        return total / count, lax.rsqrt(jnp.maximum(square - total * total / count, 1.0))

    def dose_scale(total, square):
        return lax.rsqrt(jnp.maximum(square - total * total / count, 1.0))

    hstat_pair = pair(3, hstat, hstat_in)
    hprod_pair = pair(4, hprod.at[other], hprod_in)
    back = pltpu.make_async_remote_copy(
        src_ref=hres, dst_ref=hres_in.at[core], send_sem=back_send, recv_sem=back_recv.at[core],
        device_id={"genes": lax.rem(me + n - 1, n), "samples": 1}, device_id_type=MESH,
    )

    @pl.when(has_prev)
    def _():
        fwd(expr_ref, halo_expr, n).wait_recv()

        def arrive(k, carry):
            @pl.when(k != me)
            def _():
                fwd(recv.at[k], halo.at[k], k).wait_recv()

            return carry

        lax.fori_loop(0, n, arrive, 0)
        halo[me] = sendbuf[lax.rem(me + n - 1, n)]
        pack(halo, halo_expr, hpheno, hstat)

        def halo_dot(k, carry):
            at = pl.multiple_of(k * half, half)
            hprod[k] = lax.dot_general(
                hpheno[...], dose[pl.ds(at, half), :], dims, preferred_element_type=jnp.float32
            )
            return carry

        lax.fori_loop(0, 2, halo_dot, 0)
        hstat_pair.start()
        hprod_pair.start()

    dstat_pair.wait_recv()
    dstat_pair.wait_send()
    dstat[...] = dstat[...] + dstat_in[...]

    @pl.when(has_prev)
    def _():
        hstat_pair.wait_recv()
        hprod_pair.wait_recv()
        at = pl.multiple_of(core * half, half)
        sums = dstat[0:8, pl.ds(at, half)]
        scale = dose_scale(sums, dstat[8:16, pl.ds(at, half)])

        def halo_out(p, carry):
            row = pl.multiple_of(p * genes, genes)
            mean, inv = scales(hstat, hstat_in, row)
            cross = hprod[core, pl.ds(row, genes), :] + hprod_in[pl.ds(row, genes), :]
            hres[p] = ((cross - sums * mean) * scale * inv).astype(jnp.bfloat16)
            return carry

        lax.fori_loop(0, phen, halo_out, 0)
        back.start()

    lax.fori_loop(1, n, own_arrive, 0)
    recv[me] = sendbuf[me]
    pack(recv, expr_ref, pheno, pstat)
    pstat_pair = pair(1, pstat, pstat_in)

    prod[:, rows:] = jnp.zeros((all_rows, SPILL), jnp.float32)

    def own_dot(k, carry):
        at = pl.multiple_of(k * chunk, chunk)
        prod[:, pl.ds(at, chunk)] = lax.dot_general(
            pheno[...], dose[pl.ds(at, chunk), :], dims, preferred_element_type=jnp.float32
        )
        return carry

    lax.fori_loop(0, rows // chunk, own_dot, 0)
    pstat_pair.start()

    def select_out(p, carry):
        row = pl.multiple_of(p * genes, genes)
        for t, tile in enumerate(windows(prod, row, other * width)):
            sel_out[pl.ds(row, genes), t * LANE : (t + 1) * LANE] = tile
        return carry

    lax.fori_loop(0, phen, select_out, 0)
    sel_pair = pair(2, sel_out, sel_in)
    sel_pair.start()

    pstat_pair.wait_recv()
    sel_pair.wait_recv()
    win_sum = windows(dstat, 0, core * width)
    win_square = windows(dstat, 8, core * width)
    for t in range(width // LANE):
        cols = slice(t * LANE, (t + 1) * LANE)
        win[0:8, cols] = win_sum[t]
        win[8:16, cols] = dose_scale(win_sum[t], win_square[t])

    def own_out(p, carry):
        row = pl.multiple_of(p * genes, genes)
        mean, inv = scales(pstat, pstat_in, row)
        for t, tile in enumerate(windows(prod, row, core * width)):
            cols = slice(t * LANE, (t + 1) * LANE)
            cross = tile + sel_in[pl.ds(row, genes), cols]
            own_res[pl.ds(row, genes), cols] = (cross - win[0:8, cols] * mean) * win[8:16, cols] * inv
        return carry

    lax.fori_loop(0, phen, own_out, 0)
    takes_halo = jnp.logical_and(has_next, core == 1)

    @pl.when(takes_halo)
    def _():
        for side in range(2):
            pltpu.make_async_remote_copy(
                src_ref=hres, dst_ref=hres_in.at[side], send_sem=back_send,
                recv_sem=back_recv.at[side],
                device_id={"genes": lax.rem(me + n - 1, n), "samples": 1}, device_id_type=MESH,
            ).wait_recv()
        halo_full[:, :width] = jnp.zeros((all_rows, width), jnp.float32)

        def widen(p, carry):
            row = pl.multiple_of(p * genes, genes)
            for side in range(2):
                halo_full[pl.ds(row, genes), width + side * half : width + (side + 1) * half] = (
                    hres_in[side, p].astype(jnp.float32)
                )
            return carry

        lax.fori_loop(0, phen, widen, 0)

        def add_halo(p, carry):
            row = pl.multiple_of(p * genes, genes)
            for t, tile in enumerate(windows(halo_full, row, 0)):
                cols = slice(t * LANE, (t + 1) * LANE)
                out_ref[lax.rem(p + 1, phen), :, cols] = (
                    own_res[pl.ds(row, genes), cols] + tile
                ).astype(jnp.bfloat16)
            return carry

        lax.fori_loop(0, phen, add_halo, 0)

    @pl.when(jnp.logical_not(takes_halo))
    def _():
        def plain(p, carry):
            row = pl.multiple_of(p * genes, genes)
            out_ref[lax.rem(p + 1, phen)] = own_res[pl.ds(row, genes), :].astype(jnp.bfloat16)
            return carry

        lax.fori_loop(0, phen, plain, 0)

    def drain(k, carry):
        a2a(lax.rem(me + k, n), me).wait_send()
        return carry

    lax.fori_loop(1, n, drain, 0)

    def drain_ext(k, carry):
        @pl.when(extends(k))
        def _():
            ext(k).wait_send()

        return carry

    lax.fori_loop(0, n, drain_ext, 0)
    pstat_pair.wait_send()
    sel_pair.wait_send()

    @pl.when(has_next)
    def _():
        fwd(expr_ref, halo_expr, n).wait_send()

        def drain_fwd(k, carry):
            @pl.when(relayed(k, me))
            def _():
                fwd(recv.at[k], halo.at[k], k).wait_send()

            return carry

        lax.fori_loop(0, n, drain_fwd, 0)

    @pl.when(has_prev)
    def _():
        hstat_pair.wait_send()
        hprod_pair.wait_send()
        back.wait_send()


def shards(dosage, expression, intron_counts, cluster_sizes, valid_mask, gene_block, window_start):
    n = lax.axis_size("genes")
    rows, samp = dosage.shape
    genes = expression.shape[0]
    slots = valid_mask.shape[1]
    blk = intron_counts.shape[0]
    phen = slots + 1
    all_rows = phen * genes
    width = rows // 2
    half = SPILL // 2
    vmem = pl.BlockSpec(memory_space=pltpu.VMEM)
    smem = pl.BlockSpec(memory_space=pltpu.SMEM)
    f32, bf16 = jnp.float32, jnp.bfloat16
    dma = pltpu.SemaphoreType.DMA
    result = pl.pallas_call(
        functools.partial(kernel, n, genes, slots),
        out_shape=jax.ShapeDtypeStruct((phen, genes, width), bf16),
        in_specs=[smem, smem, vmem, vmem, vmem, vmem, pl.BlockSpec(memory_space=pl.ANY)],
        out_specs=vmem,
        scratch_shapes=[
            pltpu.VMEM((rows, samp), bf16),
            pltpu.VMEM((2, n * genes, slots), f32),
            pltpu.VMEM((n * genes, slots, blk), f32),
            pltpu.VMEM((slots * genes, blk), f32),
            pltpu.VMEM((n, slots * genes, blk), bf16),
            pltpu.VMEM((n, slots * genes, blk), bf16),
            pltpu.VMEM((n, slots * genes, blk), bf16),
            pltpu.VMEM((genes, samp), bf16),
            pltpu.VMEM((all_rows, samp), bf16),
            pltpu.VMEM((all_rows, samp), bf16),
            pltpu.VMEM((all_rows, rows + SPILL), f32),
            pltpu.VMEM((2, all_rows, half), f32),
            pltpu.VMEM((all_rows, half), f32),
            pltpu.VMEM((all_rows, width), f32),
            pltpu.VMEM((all_rows, width), f32),
            pltpu.VMEM((all_rows, width), f32),
            pltpu.VMEM((all_rows, width + SPILL), f32),
            pltpu.VMEM((16, rows + SPILL), f32),
            pltpu.VMEM((16, rows + SPILL), f32),
            pltpu.VMEM((2, all_rows, LANE), f32),
            pltpu.VMEM((2, all_rows, LANE), f32),
            pltpu.VMEM((2, all_rows, LANE), f32),
            pltpu.VMEM((2, all_rows, LANE), f32),
            pltpu.VMEM((phen, genes, half), bf16),
            pltpu.VMEM((2, phen, genes, half), bf16),
            pltpu.VMEM((16, width), f32),
            dma, dma((n,)), dma((n,)), dma((n + 1,)), dma((n + 1,)), dma((5,)), dma((5,)),
            dma, dma((2,)), dma((n,)),
        ],
        compiler_params=pltpu.CompilerParams(
            collective_id=0, has_side_effects=True, vmem_limit_bytes=62 * 1024 * 1024
        ),
    )(window_start, gene_block, intron_counts, cluster_sizes.T, valid_mask.T, expression, dosage)
    return jnp.transpose(result, (1, 0, 2))


def solution(mesh):
    in_specs = (
        P(("parts", "genes"), "samples"),
        P(("parts", "genes"), "samples"),
        P(("parts", "samples", "genes"), None),
        P("parts", None),
        P("parts", None),
        P("parts"),
        P(("parts", "genes")),
    )
    out_specs = P(("parts", "genes"), None, "samples")
    return jax.shard_map(shards, mesh=mesh, in_specs=in_specs, out_specs=out_specs, check_vma=False)
```
